32 devices in a mesh: dom: 2 (over x), shard: 16 (over z, y, core).
Axes of the slice: x: 2, y: 2, z: 4, core: 2. Of those that a mesh axis runs over, the one named last changes fastest.
Arguments:
- activations: bfloat16 [4096, 8192], P(('dom', 'shard')), parts along dimension 0, may hold values from -6 to 6
- out_grads: bfloat16 [4096, 28672], P(('dom', 'shard')), parts along dimension 0, may hold values from -6 to 6
- example_ids: int32 [32, 128], P(('dom', 'shard')), parts along dimension 0, may hold values from 0 to 7, never falling along the last dimension, each value on 1 to 32 neighbouring positions
- in_factor: bfloat16 [64, 8192], P(None, 'shard'), may hold values from -0.0625 to 0.0625
- out_factor: bfloat16 [64, 28672], P(None, 'shard'), may hold values from -0.03125 to 0.03125
- query_grads: float32 [128, 4096], P('shard'), may hold values from -6 to 6
- basis_in: float32 [64, 64], replicated, may hold values from -0.75 to 0.75
- basis_out: float32 [64, 64], replicated, may hold values from -0.75 to 0.75
- eigen: float32 [64, 64], replicated, may hold values from 0.5 to 4
Outputs:
- scores: float32 [256, 128], P('dom', 'shard'), parts along dimension 0
The draws below stay inside these ranges and needn't reach their ends.
There are 2 independent parts, one for each index of `dom`. The reference program is written for one: setup_inputs(seed, part) draws one part's arguments, and reference() takes and returns one part's arrays. A program takes and returns all parts, laid end to end along the dimension named above; an argument that names none is the same for every part. Nothing has to cross between parts.
Inputs may be any that keep to these rules, and one draw needn't show every extreme that they name: `example_ids`: in each row (the 128 tokens of one shard) the example numbers never fall, and every number from 0 to 7 covers 1 to 32 tokens.
All inputs are finite; a program needn't handle non-finite values.
Results may differ from the reference program's by a relative error of at most 0.005.
Values may be sent and summed in bfloat16 or wider, within the bound.
No kernel may reach another device: no remote copies, remote signals or barrier semaphores. Data moves between devices by JAX's collectives and lax.ppermute only.
A program may use at most 128 MiB of HBM per device.

```python
import math
import jax
import jax.numpy as jnp
import numpy as np
from jax import lax

D = 8192
FF = 28672
RANK = 64
TOK_DEV = 128
EX_DEV = 8
MOST = 32
TOKENS = 2048
QUERIES = 128
N_SHARD = 16


def block_scale(own_key, dims, pieces, smallest, top_value):
    loudness = 1.0
    for dim, shards_of in pieces:
        steps = jax.random.uniform(jax.random.fold_in(jax.random.fold_in(own_key, 6), dim), (shards_of,), jnp.float32, smallest / len(pieces), top_value / len(pieces))
        loudness = loudness * jnp.repeat(jnp.exp(steps), dims[dim] // shards_of).reshape((-1,) + (1,) * (len(dims) - 1 - dim))
    return loudness


def split_up(count, total, bound, skew):
    loads = [(1 << 20) // math.isqrt(standing ** skew) + 1 for standing in range(2, count + 1)]
    rest, counts = total - bound - (count - 1), [1] * (count - 1)
    while rest > 0:
        free = [i for i in range(count - 1) if counts[i] < bound]
        pool, budget = sum([loads[i] for i in free]), rest
        for i in free:
            extra = min(bound - counts[i], max(1, budget * loads[i] // pool), rest)
            counts[i] = counts[i] + extra
            rest = rest - extra
    return np.array([bound] + counts)


def ragged(stream_key, number_of, total, limit, lean):
    if number_of == 2:
        one = jax.random.randint(stream_key, (), max(1, total - limit), min(limit, total - 1) + 1)
        return jnp.stack([one, total - one])
    sizes = jnp.asarray(split_up(number_of, total, limit, lean), jnp.int32)
    twos = (number_of - 1) // 2
    donor, sink = sizes[1:1 + 2 * twos:2], sizes[2:2 + 2 * twos:2]
    room = jnp.minimum(donor - 1, limit - sink)
    shifted = jax.random.randint(jax.random.fold_in(stream_key, 1), (twos,), 0, 1 << 20) % (room + 1)
    sizes = sizes.at[1:1 + 2 * twos:2].set(donor - shifted).at[2:2 + 2 * twos:2].set(sink + shifted)
    return sizes[jax.random.permutation(jax.random.fold_in(stream_key, 2), number_of)]


def gaussian(rng, shape, deviation, limit, shards=(), kind=jnp.bfloat16):
    entries = jax.random.normal(rng, shape, jnp.float32) * deviation
    if len(shards) > 0:
        entries = block_scale(rng, shape, shards, -0.22, 0.18) * entries
    return jnp.clip(entries, min=-limit, max=limit).astype(kind)


def setup_inputs(seed: int = 0, part: int = 0) -> dict:
    splits = jax.random.split(jax.random.key(seed), 10)
    part_keys = jax.random.split(jax.random.fold_in(splits[9], part), 10)
    return {
        "activations": gaussian(part_keys[0], (TOKENS, D), 1.0, 6.0, ((0, 16),)),
        "out_grads": gaussian(part_keys[1], (TOKENS, FF), 1.0, 6.0, ((0, 16),)),
        "example_ids": jax.vmap(lambda own: jnp.searchsorted(jnp.cumsum(ragged(own, EX_DEV, TOK_DEV, MOST, 1)), jnp.arange(TOK_DEV), side="right"))(jax.random.split(part_keys[2], N_SHARD)).reshape((N_SHARD, TOK_DEV)).astype(jnp.int32),
        "in_factor": gaussian(splits[3], (RANK, D), D ** -0.5, 0.0625, ((1, 16),)),
        "out_factor": gaussian(splits[4], (RANK, FF), FF ** -0.5, 0.03125, ((1, 16),)),
        "query_grads": gaussian(splits[5], (QUERIES, RANK * RANK), 1.0, 6.0, ((0, 16),), jnp.float32),
        "basis_in": gaussian(splits[6], (RANK, RANK), RANK ** -0.5, 0.75, (), jnp.float32),
        "basis_out": gaussian(splits[7], (RANK, RANK), RANK ** -0.5, 0.75, (), jnp.float32),
        "eigen": jnp.clip(jnp.exp(jax.random.uniform(splits[8], (RANK, RANK), jnp.float32, math.log(0.5), math.log(4.0))), 0.5, 4.0),
    }


def per_example(proj_in, proj_out, ids, groups):
    member = (ids[None, :] == jnp.arange(groups, dtype=jnp.int32)[:, None]).astype(jnp.float32)
    weighted = member[:, :, None] * proj_in.astype(jnp.float32)[None, :, :]
    blocks = jnp.einsum("eti,tj->eij", weighted, proj_out.astype(jnp.float32), precision=lax.Precision.HIGHEST)
    return blocks.reshape(groups, -1)


def precondition(query_grads, basis_in, basis_out, eigen):
    rank = basis_in.shape[0]
    grads = query_grads.reshape(-1, rank, rank)
    rotated = jnp.einsum("ai,qab,bj->qij", basis_in, grads, basis_out, precision=lax.Precision.HIGHEST)
    scaled = rotated / eigen
    restored = jnp.einsum("ia,qab,jb->qij", basis_in, scaled, basis_out, precision=lax.Precision.HIGHEST)
    return restored.reshape(grads.shape[0], -1).astype(jnp.bfloat16)


def reference(activations, out_grads, example_ids, in_factor, out_factor, query_grads, basis_in, basis_out, eigen):
    feature_blocks = activations.reshape(N_SHARD, TOK_DEV, D)
    grad_blocks = out_grads.reshape(N_SHARD, TOK_DEV, FF)

    def one_shard(items):
        features, grads, ids = items
        proj_in = jnp.dot(features, in_factor.T, preferred_element_type=jnp.float32).astype(jnp.bfloat16)
        proj_out = jnp.dot(grads, out_factor.T, preferred_element_type=jnp.float32).astype(jnp.bfloat16)
        return per_example(proj_in, proj_out, ids, EX_DEV)

    example_grads = lax.map(one_shard, (feature_blocks, grad_blocks, example_ids))
    example_grads = example_grads.reshape(N_SHARD * EX_DEV, RANK * RANK)
    precond = precondition(query_grads, basis_in, basis_out, eigen)
    scores = jnp.dot(example_grads, precond.astype(jnp.float32).T, precision=lax.Precision.HIGHEST)
    return scores * 0.00390625
```

```python
import functools
import math

import jax
import jax.numpy as jnp
from jax import lax
from jax.experimental import pallas as pl
from jax.experimental.pallas import tpu as pltpu
from jax.sharding import PartitionSpec as P

EX_DEV = 8
SCALE = 0.00390625


def grid_of(n):
    chips = n // 2
    far = 1 << -(-int(math.log2(chips)) // 2)
    return far, chips // far, 2


def moved(value, n, offset):
    return lax.ppermute(value, "shard", [(i, i ^ offset) for i in range(n)])


def precondition(query_grads, basis_in, basis_out, eigen):
    rank = basis_in.shape[0]
    grads = query_grads.reshape(-1, rank, rank)
    rotated = jnp.einsum(
        "ai,qab,bj->qij", basis_in, grads, basis_out, precision=lax.Precision.HIGHEST
    )
    scaled = rotated / eigen
    restored = jnp.einsum(
        "ia,qab,jb->qij", basis_in, scaled, basis_out, precision=lax.Precision.HIGHEST
    )
    return restored.astype(jnp.bfloat16)


NT = (((1,), (1,)), ((), ()))


def project_kernel(offsets, final, w_in, w_out, *refs):
    count = len(offsets)
    act, grad = refs[:2]
    pieces = refs[2 : 2 + count]
    at = 2 + count
    if final:
        part_in, part_out, ids = refs[at : at + 3]
        at += 3
        outs = refs[at : at + 1]
        at += 1
    else:
        outs = refs[at : at + 2]
        at += 2
    buf_in, buf_out, sem = refs[at:]
    me = lax.axis_index("shard")
    copies = []
    for k, offset in enumerate(offsets):
        src = me ^ offset
        copies.append(
            (
                pltpu.make_async_copy(
                    act.at[:, pl.ds(pl.multiple_of(src * w_in, 128), w_in)], buf_in.at[k], sem.at[k, 0]
                ),
                pltpu.make_async_copy(
                    grad.at[:, pl.ds(pl.multiple_of(src * w_out, 128), w_out)], buf_out.at[k], sem.at[k, 1]
                ),
            )
        )
    for pair in copies:
        for copy in pair:
            copy.start()
    if final:
        sum_in, sum_out = part_in[...], part_out[...]
    else:
        sum_in = sum_out = 0.0
    for k in range(count):
        copies[k][0].wait()
        sum_in = sum_in + lax.dot_general(
            pieces[k][:, :w_in], buf_in[k], NT, preferred_element_type=jnp.float32
        )
        copies[k][1].wait()
        sum_out = sum_out + lax.dot_general(
            pieces[k][:, w_in:], buf_out[k], NT, preferred_element_type=jnp.float32
        )
    if final:
        rank = sum_in.shape[0]
        outs[0][:rank] = sum_in.astype(jnp.bfloat16)
        outs[0][rank : 2 * rank] = sum_out.astype(jnp.bfloat16)
        outs[0][2 * rank :] = jnp.broadcast_to(ids[...].astype(jnp.float32), (16, ids.shape[1])).astype(
            jnp.bfloat16
        )
    else:
        outs[0][...] = sum_in
        outs[1][...] = sum_out


def project_plain(act, grad, pieces, offsets, w_in, w_out, parts, ids):
    me = lax.axis_index("shard")
    sums = list(parts) if parts is not None else [0.0, 0.0]
    for piece, offset in zip(pieces, offsets):
        src = me ^ offset
        for i, (rows, part, width) in enumerate(((act, piece[:, :w_in], w_in), (grad, piece[:, w_in:], w_out))):
            cols = lax.dynamic_slice_in_dim(rows, src * width, width, axis=1)
            sums[i] = sums[i] + lax.dot_general(part, cols, NT, preferred_element_type=jnp.float32)
    if parts is None:
        return sums
    numbers = jnp.broadcast_to(ids, (16, ids.shape[1]))
    return jnp.concatenate([s.astype(jnp.bfloat16) for s in (*sums, numbers)], axis=0)


def project(act, grad, pieces, offsets, w_in, w_out, parts=None, ids=None):
    tokens = act.shape[0]
    rank = pieces[0].shape[0]
    count = len(offsets)
    final = parts is not None
    if w_in % 128 or w_out % 128:
        return project_plain(act, grad, pieces, offsets, w_in, w_out, parts, ids)
    vmem = pl.BlockSpec(memory_space=pltpu.VMEM)
    hbm = pl.BlockSpec(memory_space=pl.ANY)
    extra = (*parts, ids) if final else ()
    if final:
        shapes = jax.ShapeDtypeStruct((2 * rank + 16, tokens), jnp.bfloat16)
        out_specs = vmem
    else:
        shapes = (jax.ShapeDtypeStruct((rank, tokens), jnp.float32),) * 2
        out_specs = (vmem, vmem)
    return pl.pallas_call(
        functools.partial(project_kernel, tuple(offsets), final, w_in, w_out),
        out_shape=shapes,
        in_specs=[hbm, hbm] + [vmem] * (count + len(extra)),
        out_specs=out_specs,
        scratch_shapes=[
            pltpu.VMEM((count, tokens, w_in), jnp.bfloat16),
            pltpu.VMEM((count, tokens, w_out), jnp.bfloat16),
            pltpu.SemaphoreType.DMA((count, 2)),
        ],
        cost_estimate=pl.CostEstimate(
            flops=2 * rank * tokens * (w_in + w_out) * count,
            bytes_accessed=2 * tokens * (w_in + w_out) * count,
            transcendentals=0,
        ),
        name="project_last" if final else "project_early",
    )(act, grad, *pieces, *extra)


def score_kernel(offsets, query, blocks, out, stacked, member):
    rank = query.shape[1]
    queries = query.shape[0] // rank
    tokens = blocks.shape[1]
    rows = 2 * rank + 16
    me = lax.axis_index("shard")
    examples = out.shape[1]
    group = stacked.shape[1] // tokens
    lane = lax.broadcasted_iota(jnp.int32, (examples, tokens), 0)
    total = 0.0
    for first in range(0, len(offsets), group):
        for k in range(group):
            base = (first + k) * rows
            turned = jnp.dot(query[...], blocks[base : base + rank], preferred_element_type=jnp.float32)
            grads = blocks[base + rank : base + 2 * rank].astype(jnp.float32)
            each = jnp.sum(turned.reshape(queries, rank, tokens) * grads[None], axis=1)
            ids = blocks[base + 2 * rank : base + rows].astype(jnp.float32)[:1].astype(jnp.int32)
            owner = ids + (me ^ offsets[first + k]) * EX_DEV
            cols = pl.ds(k * tokens, tokens)
            member[:, cols] = jnp.where(lane == owner, 1.0, 0.0).astype(jnp.bfloat16)
            high = each.astype(jnp.bfloat16).astype(jnp.float32)
            mid = (each - high).astype(jnp.bfloat16).astype(jnp.float32)
            stacked[0:queries, cols] = high
            stacked[queries : 2 * queries, cols] = mid
            stacked[2 * queries :, cols] = each - high - mid
        sums = lax.dot_general(
            stacked[...].astype(jnp.bfloat16), member[...], NT, preferred_element_type=jnp.float32
        )
        total = total + (sums[:queries] + (sums[queries : 2 * queries] + sums[2 * queries :]))
    out[...] = total * SCALE


def score(query, blocks, offsets, queries, examples):
    tokens = blocks.shape[1]
    group = math.gcd(16, len(offsets))
    vmem = pl.BlockSpec(memory_space=pltpu.VMEM)
    return pl.pallas_call(
        functools.partial(score_kernel, tuple(offsets)),
        out_shape=jax.ShapeDtypeStruct((queries, examples), jnp.float32),
        in_specs=[vmem, vmem],
        out_specs=vmem,
        scratch_shapes=[
            pltpu.VMEM((3 * queries, group * tokens), jnp.float32),
            pltpu.VMEM((examples, group * tokens), jnp.bfloat16),
        ],
        name="score",
    )(query, blocks)


def on_device(
    n,
    activations,
    out_grads,
    example_ids,
    in_factor,
    out_factor,
    query_grads,
    basis_in,
    basis_out,
    eigen,
):
    rank = in_factor.shape[0]
    far, near, cores = grid_of(n)
    fars = [k * near * cores for k in range(1, far)]
    nears = [k * cores for k in range(1, near)]
    w_in, w_out = in_factor.shape[1], out_factor.shape[1]
    own = jnp.concatenate([in_factor, out_factor], axis=1)
    pieces = {0: own}
    order = []
    for f in [0] + fars:
        if f:
            pieces[f] = moved(own, n, f)
        order.append(f)
        for m in nears:
            pieces[f ^ m] = moved(pieces[f], n, m)
            order.append(f ^ m)
    full = []
    for o in order:
        pieces[o ^ 1] = moved(pieces[o], n, 1)
        full += [o, o ^ 1]
    last = full[-2 * len(nears) :]
    early = full[: -2 * len(nears)]
    parts = project(activations, out_grads, [pieces[o] for o in early], early, w_in, w_out)
    mine = project(
        activations, out_grads, [pieces[o] for o in last], last, w_in, w_out, parts, example_ids
    )
    query = precondition(query_grads, basis_in, basis_out, eigen)
    queries = query.shape[0]
    query = query.transpose(0, 2, 1).reshape(queries * rank, rank)
    offsets = [0] + fars
    row = jnp.concatenate([mine] + [moved(mine, n, f) for f in fars], axis=0)
    plane = jnp.concatenate([row] + [moved(row, n, m) for m in nears], axis=0)
    offsets = [o ^ m for m in [0] + nears for o in offsets]
    blocks = jnp.concatenate([plane, moved(plane, n, 1)], axis=0)
    offsets = offsets + [o ^ 1 for o in offsets]
    return score(query, blocks, offsets, queries, EX_DEV * n).T


def solution(mesh):
    placed = (
        P(("dom", "shard"), None),
        P(("dom", "shard"), None),
        P(("dom", "shard"), None),
        P(None, "shard"),
        P(None, "shard"),
        P("shard", None),
        P(),
        P(),
        P(),
    )
    return jax.shard_map(
        functools.partial(on_device, mesh.shape["shard"]),
        mesh=mesh,
        in_specs=placed,
        out_specs=P("dom", "shard"),
        check_vma=False,
    )
```

```python
import functools
import math

import jax
import jax.numpy as jnp
from jax import lax
from jax.experimental import pallas as pl
from jax.experimental.pallas import tpu as pltpu
from jax.sharding import PartitionSpec as P


EX_DEV = 8
SCALE = 0.00390625


def grid_of(n):
    chips = n // 2
    far = 1 << -(-int(math.log2(chips)) // 2)
    return far, chips // far, 2


def moved(value, n, offset):
    return lax.ppermute(value, "shard", [(i, i ^ offset) for i in range(n)])


NT = (((1,), (1,)), ((), ()))
VMEM = pl.BlockSpec(memory_space=pltpu.VMEM)
HBM = pl.BlockSpec(memory_space=pltpu.HBM)
MIB = 1 << 20


def columns(ref, first, width):
    return ref.at[:, pl.ds(pl.multiple_of(first * width, 128), width)]


def run_copies(pairs, sems):
    copies = [pltpu.make_async_copy(src, dst, sems.at[i]) for i, (src, dst) in enumerate(pairs)]
    for copy in copies:
        copy.start()
    for copy in copies:
        copy.wait()


def split_kernel(inner, outer, mine, sems):
    h_in, h_out = inner.shape[1] // 2, outer.shape[1] // 2
    dom = lax.axis_index("dom") % 2
    run_copies(
        [(columns(inner, dom, h_in), mine.at[:, :h_in]), (columns(outer, dom, h_out), mine.at[:, h_in:])], sems
    )


def split(in_factor, out_factor):
    rank = in_factor.shape[0]
    width = (in_factor.shape[1] + out_factor.shape[1]) // 2
    return pl.pallas_call(
        split_kernel,
        out_shape=jax.ShapeDtypeStruct((rank, width), in_factor.dtype),
        in_specs=[HBM, HBM],
        out_specs=VMEM,
        scratch_shapes=[pltpu.SemaphoreType.DMA((2,))],
        cost_estimate=pl.CostEstimate(flops=2 * 10**10, bytes_accessed=0, transcendentals=0),
        compiler_params=pltpu.CompilerParams(vmem_limit_bytes=2 * MIB),
        name="split",
    )(in_factor, out_factor)


INNER, OUTER, CARRIED, CROSSED = range(4)


def project_kernel(keys, h_in, has_part, final, act, grad, *refs):
    count = len(keys)
    pieces = refs[:count]
    out = refs[-1]
    rank = pieces[0].shape[0]
    me = lax.axis_index("shard")
    dom = lax.axis_index("dom") % 2
    part = refs[count][...] if has_part else None
    sums = [part[:, :rank], part[:, rank:]] if has_part else [0.0, 0.0]

    def add(j, piece, place, lo, size):
        rows = (act, grad)[j][:, pl.ds(pl.multiple_of(place * size, 128), size)]
        sums[j] = sums[j] + lax.dot_general(
            rows, piece[:, lo : lo + size], NT, preferred_element_type=jnp.float32
        )

    for piece, (offset, kind) in zip(pieces, keys):
        src = me ^ offset
        width = piece.shape[1]
        if kind in (INNER, OUTER):
            add(kind, piece, src, 0, width)
        else:
            place = 2 * src + (dom if kind == CARRIED else 1 - dom)
            add(INNER, piece, place, 0, h_in)
            add(OUTER, piece, place, h_in, width - h_in)
    total = jnp.concatenate(sums, axis=1)
    if final:
        ids = refs[count + 1]
        out[: 2 * rank] = total.T.astype(jnp.bfloat16)
        out[2 * rank :] = jnp.broadcast_to(ids[...].astype(jnp.float32), (16, ids.shape[1])).astype(jnp.bfloat16)
    else:
        out[...] = total


def project(act, grad, pieces, keys, h_in, part, ids):
    tokens = act.shape[0]
    rank = pieces[0].shape[0]
    extra = (() if part is None else (part,)) + (() if ids is None else (ids,))
    if ids is None:
        shape = jax.ShapeDtypeStruct((tokens, 2 * rank), jnp.float32)
    else:
        shape = jax.ShapeDtypeStruct((2 * rank + 16, tokens), jnp.bfloat16)
    size = sum(piece.size for piece in pieces)
    return pl.pallas_call(
        functools.partial(project_kernel, tuple(keys), h_in, part is not None, ids is not None),
        out_shape=shape,
        in_specs=[VMEM] * (2 + len(pieces) + len(extra)),
        out_specs=VMEM,
        cost_estimate=pl.CostEstimate(
            flops=2 * tokens * size, bytes_accessed=2 * tokens * size // rank, transcendentals=0
        ),
        compiler_params=pltpu.CompilerParams(vmem_limit_bytes=3 * MIB),
    )(act, grad, *pieces, *extra)


def project_halves(n, act, grad, ids, in_factor, out_factor):
    far, near, cores = grid_of(n)
    fars = [k * near * cores for k in range(1, far)]
    nears = [k * cores for k in range(1, near)]
    h_in = in_factor.shape[1] // 2

    def crossed(value):
        return lax.ppermute(value, "dom", [(0, 1), (1, 0)])

    mine = split(in_factor, out_factor)
    held = {(0, INNER): in_factor, (0, OUTER): out_factor}

    def bring(key, source, offset):
        held[key] = moved(held[source] if source in held else mine, n, offset)

    near_keys = []
    for m in nears:
        bring((m, CARRIED), (0, CARRIED), m)
        held[m, CROSSED] = crossed(held[m, CARRIED])
        near_keys += [(m, CARRIED), (m, CROSSED)]
    waves = []
    for i, f in enumerate(fars):
        wave = []
        for kind in (INNER, OUTER) if i == 0 else (CARRIED,):
            bring((f, kind), (0, kind), f)
            wave.append((f, kind))
            for m in nears:
                bring((f ^ m, kind), (f, kind), m)
                wave.append((f ^ m, kind))
        if i:
            for o, _ in list(wave):
                held[o, CROSSED] = crossed(held[o, CARRIED])
            wave += [(o, CROSSED) for o, _ in wave]
        waves.append(wave)
    for o, kind in list(held):
        held[o ^ 1, kind] = moved(held[o, kind], n, 1)
    rest = [key for wave in waves[1:] for key in wave]
    late = [key for key in rest[len(rest) // 2 - len(nears) :] if key != waves[-1][0]]
    groups = [[(0, INNER), (0, OUTER)], near_keys + waves[0], [key for key in rest if key not in late]]
    groups += [late[:-1], late[-1:]]
    part = None
    for i, keys in enumerate(groups):
        keys = [(o ^ c, kind) for o, kind in keys for c in (0, 1)]
        last = ids if i == len(groups) - 1 else None
        part = project(act, grad, [held[key] for key in keys], keys, h_in, part, last)
    return part


def project_plain(n, act, grad, ids, in_factor, out_factor):
    w_in, w_out = in_factor.shape[1], out_factor.shape[1]
    pieces = [jnp.concatenate([in_factor, out_factor], axis=1)]
    offsets = [0]
    step = n // 2
    while step:
        pieces += [moved(piece, n, step) for piece in pieces]
        offsets += [offset ^ step for offset in offsets]
        step //= 2
    me = lax.axis_index("shard")
    sums = [0.0, 0.0]
    for piece, offset in zip(pieces, offsets):
        src = me ^ offset
        for i, (rows, part, width) in enumerate(((act, piece[:, :w_in], w_in), (grad, piece[:, w_in:], w_out))):
            cols = lax.dynamic_slice_in_dim(rows, src * width, width, axis=1)
            sums[i] = sums[i] + lax.dot_general(part, cols, NT, preferred_element_type=jnp.float32)
    numbers = jnp.broadcast_to(ids, (16, ids.shape[1]))
    return jnp.concatenate([s.astype(jnp.bfloat16) for s in (*sums, numbers)], axis=0)


def halves_of(value):
    high = value.astype(jnp.bfloat16)
    return high, (value - high.astype(jnp.float32)).astype(jnp.bfloat16)


def fine_dot(left, right, dims):
    dot = functools.partial(lax.dot_general, dimension_numbers=dims, preferred_element_type=jnp.float32)
    (a, a_rest), (b, b_rest) = halves_of(left), halves_of(right)
    return dot(a, b) + (dot(a, b_rest) + dot(a_rest, b))


def precondition_kernel(grads, basis_in, basis_out, eigen, out, stacked, turned):
    rank = basis_in.shape[0]
    queries = grads.shape[0]
    nn = (((1,), (0,)), ((), ()))
    for a in range(rank):
        stacked[pl.ds(a, queries, stride=rank)] = grads[:, a * rank : (a + 1) * rank]
    inner, outer, weights = basis_in[...], basis_out[...], eigen[...]
    inner_t = inner.T
    right = fine_dot(stacked[...], outer, nn)
    parts = [right[q * rank : (q + 1) * rank] for q in range(queries)]
    scaled = [fine_dot(inner_t, part, nn) / weights for part in parts]
    back = fine_dot(jnp.concatenate(scaled, axis=0), outer, NT)
    for q in range(queries):
        turned[pl.ds(q, rank, stride=queries)] = fine_dot(inner, back[q * rank : (q + 1) * rank], nn)
    out[...] = turned[...].astype(jnp.bfloat16)


def precondition(query_grads, basis_in, basis_out, eigen):
    rank = basis_in.shape[0]
    rows = query_grads.shape[0] * rank
    return pl.pallas_call(
        precondition_kernel,
        out_shape=jax.ShapeDtypeStruct((rows, rank), jnp.bfloat16),
        in_specs=[VMEM] * 4,
        out_specs=VMEM,
        scratch_shapes=[pltpu.VMEM((rows, rank), jnp.float32)] * 2,
        cost_estimate=pl.CostEstimate(
            flops=10**10, bytes_accessed=4 * rows * rank, transcendentals=0
        ),
        compiler_params=pltpu.CompilerParams(vmem_limit_bytes=8 * MIB),
        name="precondition",
    )(query_grads, basis_in, basis_out, eigen)


def score_kernel(offsets, final, has_part, query, *refs):
    count = len(offsets)
    blocks = refs[:count]
    out, stacked, member = refs[-3:]
    rank = query.shape[1]
    queries = query.shape[0] // rank
    tokens = blocks[0].shape[1]
    me = lax.axis_index("shard")
    examples = out.shape[1]
    group = stacked.shape[1] // tokens
    lane = lax.broadcasted_iota(jnp.int32, (examples, tokens), 0)
    total = refs[count][...] if has_part else 0.0
    for first in range(0, count, group):
        for k in range(group):
            block = blocks[first + k]
            turned = jnp.dot(query[...], block[rank : 2 * rank], preferred_element_type=jnp.float32)
            inputs = block[:rank].astype(jnp.float32)
            each = jnp.sum(turned.reshape(rank, queries, tokens) * inputs[:, None, :], axis=0)
            ids = block[2 * rank :].astype(jnp.float32)[:1].astype(jnp.int32)
            owner = ids + (me ^ offsets[first + k]) * EX_DEV
            cols = pl.ds(k * tokens, tokens)
            member[:, cols] = jnp.where(lane == owner, 1.0, 0.0).astype(jnp.bfloat16)
            high = each.astype(jnp.bfloat16).astype(jnp.float32)
            mid = (each - high).astype(jnp.bfloat16).astype(jnp.float32)
            stacked[0:queries, cols] = high
            stacked[queries : 2 * queries, cols] = mid
            stacked[2 * queries :, cols] = each - high - mid
        sums = lax.dot_general(
            stacked[...].astype(jnp.bfloat16), member[...], NT, preferred_element_type=jnp.float32
        )
        total = total + (sums[:queries] + (sums[queries : 2 * queries] + sums[2 * queries :]))
    out[...] = total * SCALE if final else total


def score(query, blocks, offsets, examples, part, final):
    rank2, tokens = blocks[0].shape
    queries = query.shape[0] // query.shape[1]
    group = math.gcd(4, len(offsets))
    parts = () if part is None else (part,)
    return pl.pallas_call(
        functools.partial(score_kernel, tuple(offsets), final, bool(parts)),
        out_shape=jax.ShapeDtypeStruct((queries, examples), jnp.float32),
        in_specs=[VMEM] * (1 + len(blocks) + len(parts)),
        out_specs=VMEM,
        scratch_shapes=[
            pltpu.VMEM((3 * queries, group * tokens), jnp.float32),
            pltpu.VMEM((examples, group * tokens), jnp.bfloat16),
        ],
        cost_estimate=pl.CostEstimate(
            flops=2 * query.size * tokens * len(blocks),
            bytes_accessed=2 * rank2 * tokens * len(blocks),
            transcendentals=0,
        ),
        compiler_params=pltpu.CompilerParams(vmem_limit_bytes=4 * MIB),
    )(query, *blocks, *parts)


def on_device(
    n,
    doms,
    activations,
    out_grads,
    example_ids,
    in_factor,
    out_factor,
    query_grads,
    basis_in,
    basis_out,
    eigen,
):
    far, near, cores = grid_of(n)
    fars = [k * near * cores for k in range(1, far)]
    nears = [k * cores for k in range(1, near)]
    aligned = doms == 2 and in_factor.shape[1] % 256 == 0 and out_factor.shape[1] % 256 == 0
    project_all = project_halves if aligned else project_plain
    mine = project_all(n, activations, out_grads, example_ids, in_factor, out_factor)
    query = precondition(query_grads, basis_in, basis_out, eigen)
    row = {0: mine}
    for i, f in reversed(list(enumerate(fars))):
        row[f] = moved(mine, n, f)
    rest = {o ^ m: moved(block, n, m) for m in nears for o, block in row.items()}
    steps = [row, {o ^ 1: moved(block, n, 1) for o, block in row.items()}]
    cores = {}
    for o, block in rest.items():
        cores[o ^ 1] = moved(block, n, 1)
    steps += [rest, cores]
    total = None
    for i, step in enumerate(steps):
        total = score(query, list(step.values()), list(step), EX_DEV * n, total, i == len(steps) - 1)
    return total.T


def solution(mesh):
    placed = (
        P(("dom", "shard"), None),
        P(("dom", "shard"), None),
        P(("dom", "shard"), None),
        P(None, "shard"),
        P(None, "shard"),
        P("shard", None),
        P(),
        P(),
        P(),
    )
    return jax.shard_map(
        functools.partial(on_device, mesh.shape["shard"], mesh.shape["dom"]),
        mesh=mesh,
        in_specs=placed,
        out_specs=P("dom", "shard"),
        check_vma=False,
    )
```

```python
import functools
import math

import jax
import jax.numpy as jnp
from jax import lax
from jax.experimental import pallas as pl
from jax.experimental.pallas import tpu as pltpu
from jax.sharding import PartitionSpec as P


EX_DEV = 8
SCALE = 0.00390625


def grid_of(n):
    chips = n // 2
    far = 1 << -(-int(math.log2(chips)) // 2)
    return far, chips // far, 2


def moved(value, n, offset):
    return lax.ppermute(value, "shard", [(i, i ^ offset) for i in range(n)])


NT = (((1,), (1,)), ((), ()))
VMEM = pl.BlockSpec(memory_space=pltpu.VMEM)
MIB = 1 << 20


def numbers_kernel(ids, out):
    out[...] = jnp.broadcast_to(ids[...].astype(jnp.float32), out.shape).astype(jnp.bfloat16)


def numbers_of(ids):
    return pl.pallas_call(
        numbers_kernel,
        out_shape=jax.ShapeDtypeStruct((16, ids.shape[1]), jnp.bfloat16),
        in_specs=[VMEM],
        out_specs=VMEM,
        cost_estimate=pl.CostEstimate(flops=2 * 10**10, bytes_accessed=0, transcendentals=0),
        compiler_params=pltpu.CompilerParams(vmem_limit_bytes=2 * MIB),
        name="numbers",
    )(ids)


INNER, OUTER = 0, 1


def project_kernel(keys, has_part, final, act, grad, *refs):
    count = len(keys)
    pieces = refs[:count]
    out = refs[-1]
    rank = pieces[0].shape[0]
    me = lax.axis_index("shard")
    even = lax.axis_index("dom") % 2 == 0
    part = refs[count][...] if has_part else None
    sums = [part[:, :rank], part[:, rank:]] if has_part else [0.0, 0.0]
    for piece, (first, second, kind) in zip(pieces, keys):
        src = me ^ (first if first == second else jnp.where(even, first, second))
        width = piece.shape[1]
        rows = (act, grad)[kind][:, pl.ds(pl.multiple_of(src * width, 128), width)]
        sums[kind] = sums[kind] + lax.dot_general(
            rows, piece[...], NT, preferred_element_type=jnp.float32
        )
    total = jnp.concatenate(sums, axis=1)
    if final:
        out[: 2 * rank] = total.T.astype(jnp.bfloat16)
        out[2 * rank :] = refs[count + 1][...]
    else:
        out[...] = total


def project(act, grad, pieces, keys, part, numbers):
    tokens = act.shape[0]
    rank = pieces[0].shape[0]
    extra = (() if part is None else (part,)) + (() if numbers is None else (numbers,))
    if numbers is None:
        shape = jax.ShapeDtypeStruct((tokens, 2 * rank), jnp.float32)
    else:
        shape = jax.ShapeDtypeStruct((2 * rank + 16, tokens), jnp.bfloat16)
    size = sum(piece.size for piece in pieces)
    return pl.pallas_call(
        functools.partial(project_kernel, tuple(keys), part is not None, numbers is not None),
        out_shape=shape,
        in_specs=[VMEM] * (2 + len(pieces) + len(extra)),
        out_specs=VMEM,
        cost_estimate=pl.CostEstimate(
            flops=2 * tokens * size, bytes_accessed=2 * tokens * size // rank, transcendentals=0
        ),
        compiler_params=pltpu.CompilerParams(vmem_limit_bytes=3 * MIB),
    )(act, grad, *pieces, *extra)


def project_paired(n, act, grad, ids, in_factor, out_factor):
    far, near, cores = grid_of(n)
    fars = [k * near * cores for k in range(1, far)]
    nears = [k * cores for k in range(1, near)]
    kinds = (OUTER, INNER)
    held = {(0, 0, INNER): in_factor, (0, 0, OUTER): out_factor}

    def bring(source, even, odd):
        to = (source[0] ^ even, source[1] ^ odd)
        pairs = [(i, i ^ even) for i in range(n)] + [(n + i, n + (i ^ odd)) for i in range(n)]
        for kind in kinds:
            held[(*to, kind)] = lax.ppermute(held[(*source, kind)], ("dom", "shard"), pairs)
        return to

    def cross(source):
        to = source[::-1]
        for kind in kinds:
            held[(*to, kind)] = lax.ppermute(held[(*source, kind)], "dom", [(0, 1), (1, 0)])
        return to

    own = (0, 0)
    first = [bring(own, m, m) for m in nears]
    nearest = bring(own, fars[0], fars[0])
    first.append(nearest)
    turned = [bring(nearest, m, m) for m in nears]
    middle, last = [], []
    for i in range(1, far - 1, 2):
        there = bring(own, fars[i], fars[i + 1])
        beside = [bring(there, m, m) for m in nears]
        middle += [there, *beside, cross(there)]
        last += [cross(to) for to in beside]
    for key in list(held):
        held[key[0] ^ 1, key[1] ^ 1, key[2]] = lax.ppermute(
            held[key], "shard", [(i, i ^ 1) for i in range(n)]
        )
    numbers = numbers_of(ids)
    part = None
    groups = ([own], first, middle, turned, last)
    for i, group in enumerate(groups):
        keys = [(a ^ c, b ^ c, kind) for a, b in group for c in (0, 1) for kind in kinds]
        rows = numbers if i == len(groups) - 1 else None
        part = project(act, grad, [held[key] for key in keys], keys, part, rows)
    return part


def project_plain(n, act, grad, ids, in_factor, out_factor):
    w_in, w_out = in_factor.shape[1], out_factor.shape[1]
    pieces = [jnp.concatenate([in_factor, out_factor], axis=1)]
    offsets = [0]
    step = n // 2
    while step:
        pieces += [moved(piece, n, step) for piece in pieces]
        offsets += [offset ^ step for offset in offsets]
        step //= 2
    me = lax.axis_index("shard")
    sums = [0.0, 0.0]
    for piece, offset in zip(pieces, offsets):
        src = me ^ offset
        for i, (rows, part, width) in enumerate(((act, piece[:, :w_in], w_in), (grad, piece[:, w_in:], w_out))):
            cols = lax.dynamic_slice_in_dim(rows, src * width, width, axis=1)
            sums[i] = sums[i] + lax.dot_general(part, cols, NT, preferred_element_type=jnp.float32)
    numbers = jnp.broadcast_to(ids, (16, ids.shape[1]))
    return jnp.concatenate([s.astype(jnp.bfloat16) for s in (*sums, numbers)], axis=0)


def halves_of(value):
    high = value.astype(jnp.bfloat16)
    return high, (value - high.astype(jnp.float32)).astype(jnp.bfloat16)


def fine_dot(left, right, dims):
    dot = functools.partial(lax.dot_general, dimension_numbers=dims, preferred_element_type=jnp.float32)
    (a, a_rest), (b, b_rest) = halves_of(left), halves_of(right)
    return dot(a, b) + (dot(a, b_rest) + dot(a_rest, b))


def precondition_kernel(grads, basis_in, basis_out, eigen, out, stacked, turned):
    rank = basis_in.shape[0]
    queries = grads.shape[0]
    nn = (((1,), (0,)), ((), ()))
    for a in range(rank):
        stacked[pl.ds(a, queries, stride=rank)] = grads[:, a * rank : (a + 1) * rank]
    inner, outer, weights = basis_in[...], basis_out[...], eigen[...]
    inner_t = inner.T
    right = fine_dot(stacked[...], outer, nn)
    parts = [right[q * rank : (q + 1) * rank] for q in range(queries)]
    scaled = [fine_dot(inner_t, part, nn) / weights for part in parts]
    back = fine_dot(jnp.concatenate(scaled, axis=0), outer, NT)
    for q in range(queries):
        turned[pl.ds(q, rank, stride=queries)] = fine_dot(inner, back[q * rank : (q + 1) * rank], nn)
    out[...] = turned[...].astype(jnp.bfloat16)


def precondition(query_grads, basis_in, basis_out, eigen):
    rank = basis_in.shape[0]
    rows = query_grads.shape[0] * rank
    return pl.pallas_call(
        precondition_kernel,
        out_shape=jax.ShapeDtypeStruct((rows, rank), jnp.bfloat16),
        in_specs=[VMEM] * 4,
        out_specs=VMEM,
        scratch_shapes=[pltpu.VMEM((rows, rank), jnp.float32)] * 2,
        cost_estimate=pl.CostEstimate(
            flops=10**10, bytes_accessed=4 * rows * rank, transcendentals=0
        ),
        compiler_params=pltpu.CompilerParams(vmem_limit_bytes=8 * MIB),
        name="precondition",
    )(query_grads, basis_in, basis_out, eigen)


def score_kernel(offsets, final, has_part, query, *refs):
    count = len(offsets)
    blocks = refs[:count]
    out, stacked, member = refs[-3:]
    rank = query.shape[1]
    queries = query.shape[0] // rank
    tokens = blocks[0].shape[1]
    me = lax.axis_index("shard")
    examples = out.shape[1]
    group = stacked.shape[1] // tokens
    lane = lax.broadcasted_iota(jnp.int32, (examples, tokens), 0)
    total = refs[count][...] if has_part else 0.0
    for first in range(0, count, group):
        for k in range(group):
            block = blocks[first + k]
            turned = jnp.dot(query[...], block[rank : 2 * rank], preferred_element_type=jnp.float32)
            inputs = block[:rank].astype(jnp.float32)
            each = jnp.sum(turned.reshape(rank, queries, tokens) * inputs[:, None, :], axis=0)
            ids = block[2 * rank :].astype(jnp.float32)[:1].astype(jnp.int32)
            owner = ids + (me ^ offsets[first + k]) * EX_DEV
            cols = pl.ds(k * tokens, tokens)
            member[:, cols] = jnp.where(lane == owner, 1.0, 0.0).astype(jnp.bfloat16)
            high = each.astype(jnp.bfloat16).astype(jnp.float32)
            mid = (each - high).astype(jnp.bfloat16).astype(jnp.float32)
            stacked[0:queries, cols] = high
            stacked[queries : 2 * queries, cols] = mid
            stacked[2 * queries :, cols] = each - high - mid
        sums = lax.dot_general(
            stacked[...].astype(jnp.bfloat16), member[...], NT, preferred_element_type=jnp.float32
        )
        total = total + (sums[:queries] + (sums[queries : 2 * queries] + sums[2 * queries :]))
    out[...] = total * SCALE if final else total


def score(query, blocks, offsets, examples, part, final):
    rank2, tokens = blocks[0].shape
    queries = query.shape[0] // query.shape[1]
    group = math.gcd(4, len(offsets))
    parts = () if part is None else (part,)
    return pl.pallas_call(
        functools.partial(score_kernel, tuple(offsets), final, bool(parts)),
        out_shape=jax.ShapeDtypeStruct((queries, examples), jnp.float32),
        in_specs=[VMEM] * (1 + len(blocks) + len(parts)),
        out_specs=VMEM,
        scratch_shapes=[
            pltpu.VMEM((3 * queries, group * tokens), jnp.float32),
            pltpu.VMEM((examples, group * tokens), jnp.bfloat16),
        ],
        cost_estimate=pl.CostEstimate(
            flops=2 * query.size * tokens * len(blocks),
            bytes_accessed=2 * rank2 * tokens * len(blocks),
            transcendentals=0,
        ),
        compiler_params=pltpu.CompilerParams(vmem_limit_bytes=4 * MIB),
    )(query, *blocks, *parts)


def on_device(
    n,
    doms,
    activations,
    out_grads,
    example_ids,
    in_factor,
    out_factor,
    query_grads,
    basis_in,
    basis_out,
    eigen,
):
    far, near, cores = grid_of(n)
    fars = [k * near * cores for k in range(1, far)]
    nears = [k * cores for k in range(1, near)]
    aligned = doms == 2 and far % 2 == 0 and in_factor.shape[1] % 128 == 0 and out_factor.shape[1] % 128 == 0
    project_all = project_paired if aligned else project_plain
    mine = project_all(n, activations, out_grads, example_ids, in_factor, out_factor)
    query = precondition(query_grads, basis_in, basis_out, eigen)
    row = {0: mine}
    for i, f in sorted(enumerate(fars), key=lambda item: (item[0] == far // 2 - 1, -item[0])):
        row[f] = moved(mine, n, f)
    rest = {o ^ m: moved(block, n, m) for m in nears for o, block in row.items()}
    steps = [row, {o ^ 1: moved(block, n, 1) for o, block in row.items()}]
    cores = {}
    for o, block in rest.items():
        cores[o ^ 1] = moved(block, n, 1)
    steps += [rest, cores]
    total = None
    for i, step in enumerate(steps):
        total = score(query, list(step.values()), list(step), EX_DEV * n, total, i == len(steps) - 1)
    return total.T


def solution(mesh):
    placed = (
        P(("dom", "shard"), None),
        P(("dom", "shard"), None),
        P(("dom", "shard"), None),
        P(None, "shard"),
        P(None, "shard"),
        P("shard", None),
        P(),
        P(),
        P(),
    )
    return jax.shard_map(
        functools.partial(on_device, mesh.shape["shard"], mesh.shape["dom"]),
        mesh=mesh,
        in_specs=placed,
        out_specs=P("dom", "shard"),
        check_vma=False,
    )
```

```python
import functools
import math

import jax
import jax.numpy as jnp
from jax import lax
from jax.experimental import pallas as pl
from jax.experimental.pallas import tpu as pltpu
from jax.sharding import PartitionSpec as P


EX_DEV = 8
SCALE = 0.00390625


def grid_of(n):
    chips = n // 2
    far = 1 << -(-int(math.log2(chips)) // 2)
    return far, chips // far, 2


def moved(value, n, offset):
    return lax.ppermute(value, "shard", [(i, i ^ offset) for i in range(n)])


NT = (((1,), (1,)), ((), ()))
VMEM = pl.BlockSpec(memory_space=pltpu.VMEM)
MIB = 1 << 20


def numbers_kernel(ids, out):
    out[...] = jnp.broadcast_to(ids[...].astype(jnp.float32), out.shape).astype(jnp.bfloat16)


def numbers_of(ids):
    return pl.pallas_call(
        numbers_kernel,
        out_shape=jax.ShapeDtypeStruct((8, ids.shape[1]), jnp.bfloat16),
        in_specs=[VMEM],
        out_specs=VMEM,
        cost_estimate=pl.CostEstimate(flops=2 * 10**10, bytes_accessed=0, transcendentals=0),
        compiler_params=pltpu.CompilerParams(vmem_limit_bytes=2 * MIB),
        name="numbers",
    )(ids)


INNER, OUTER = 0, 1


def project_kernel(keys, has_part, final, act, grad, *refs):
    count = len(keys)
    pieces = refs[:count]
    out = refs[-1]
    rank = pieces[0].shape[0]
    me = lax.axis_index("shard")
    even = lax.axis_index("dom") % 2 == 0
    part = refs[count][...] if has_part else None
    sums = [part[:, :rank], part[:, rank:]] if has_part else [0.0, 0.0]
    for piece, (first, second, kind) in zip(pieces, keys):
        src = me ^ (first if first == second else jnp.where(even, first, second))
        width = piece.shape[1]
        rows = (act, grad)[kind][:, pl.ds(pl.multiple_of(src * width, 128), width)]
        sums[kind] = sums[kind] + lax.dot_general(
            rows, piece[...], NT, preferred_element_type=jnp.float32
        )
    total = jnp.concatenate(sums, axis=1)
    if final:
        out[: 2 * rank] = total.T.astype(jnp.bfloat16)
        out[2 * rank :] = refs[count + 1][...]
    else:
        out[...] = total


def project(act, grad, pieces, keys, part, numbers):
    tokens = act.shape[0]
    rank = pieces[0].shape[0]
    extra = (() if part is None else (part,)) + (() if numbers is None else (numbers,))
    if numbers is None:
        shape = jax.ShapeDtypeStruct((tokens, 2 * rank), jnp.float32)
    else:
        shape = jax.ShapeDtypeStruct((2 * rank + 8, tokens), jnp.bfloat16)
    size = sum(piece.size for piece in pieces)
    return pl.pallas_call(
        functools.partial(project_kernel, tuple(keys), part is not None, numbers is not None),
        out_shape=shape,
        in_specs=[VMEM] * (2 + len(pieces) + len(extra)),
        out_specs=VMEM,
        cost_estimate=pl.CostEstimate(
            flops=2 * tokens * size, bytes_accessed=2 * tokens * size // rank, transcendentals=0
        ),
        compiler_params=pltpu.CompilerParams(vmem_limit_bytes=3 * MIB),
    )(act, grad, *pieces, *extra)


def project_paired(n, act, grad, ids, in_factor, out_factor):
    far, near, cores = grid_of(n)
    fars = [k * near * cores for k in range(1, far)]
    nears = [k * cores for k in range(1, near)]
    kinds = (OUTER, INNER)
    held = {(0, 0, INNER): in_factor, (0, 0, OUTER): out_factor}

    def bring(source, even, odd):
        to = (source[0] ^ even, source[1] ^ odd)
        pairs = [(i, i ^ even) for i in range(n)] + [(n + i, n + (i ^ odd)) for i in range(n)]
        for kind in kinds:
            held[(*to, kind)] = lax.ppermute(held[(*source, kind)], ("dom", "shard"), pairs)
        return to

    def cross(source):
        to = source[::-1]
        for kind in kinds:
            held[(*to, kind)] = lax.ppermute(held[(*source, kind)], "dom", [(0, 1), (1, 0)])
        return to

    own = (0, 0)
    first = [bring(own, m, m) for m in nears]
    nearest = bring(own, fars[0], fars[0])
    first.append(nearest)
    turned = [bring(nearest, m, m) for m in nears]
    middle, last = [], []
    for i in range(1, far - 1, 2):
        there = bring(own, fars[i], fars[i + 1])
        beside = [bring(there, m, m) for m in nears]
        middle += [there, *beside, cross(there)]
        last += [cross(to) for to in beside]
    for key in list(held):
        held[key[0] ^ 1, key[1] ^ 1, key[2]] = lax.ppermute(
            held[key], "shard", [(i, i ^ 1) for i in range(n)]
        )
    numbers = numbers_of(ids)
    part = None
    groups = ([own], first, middle, turned, last)
    for i, group in enumerate(groups):
        keys = [(a ^ c, b ^ c, kind) for a, b in group for c in (0, 1) for kind in kinds]
        rows = numbers if i == len(groups) - 1 else None
        part = project(act, grad, [held[key] for key in keys], keys, part, rows)
    return part


def project_plain(n, act, grad, ids, in_factor, out_factor):
    w_in, w_out = in_factor.shape[1], out_factor.shape[1]
    pieces = [jnp.concatenate([in_factor, out_factor], axis=1)]
    offsets = [0]
    step = n // 2
    while step:
        pieces += [moved(piece, n, step) for piece in pieces]
        offsets += [offset ^ step for offset in offsets]
        step //= 2
    me = lax.axis_index("shard")
    sums = [0.0, 0.0]
    for piece, offset in zip(pieces, offsets):
        src = me ^ offset
        for i, (rows, part, width) in enumerate(((act, piece[:, :w_in], w_in), (grad, piece[:, w_in:], w_out))):
            cols = lax.dynamic_slice_in_dim(rows, src * width, width, axis=1)
            sums[i] = sums[i] + lax.dot_general(part, cols, NT, preferred_element_type=jnp.float32)
    numbers = jnp.broadcast_to(ids, (8, ids.shape[1]))
    return jnp.concatenate([s.astype(jnp.bfloat16) for s in (*sums, numbers)], axis=0)


def halves_of(value):
    high = value.astype(jnp.bfloat16)
    return high, (value - high.astype(jnp.float32)).astype(jnp.bfloat16)


def fine_dot(left, right, dims):
    dot = functools.partial(lax.dot_general, dimension_numbers=dims, preferred_element_type=jnp.float32)
    (a, a_rest), (b, b_rest) = halves_of(left), halves_of(right)
    return dot(a, b) + (dot(a, b_rest) + dot(a_rest, b))


def precondition_kernel(grads, basis_in, basis_out, eigen, out, stacked, turned):
    rank = basis_in.shape[0]
    queries = grads.shape[0]
    nn = (((1,), (0,)), ((), ()))
    for a in range(rank):
        stacked[pl.ds(a, queries, stride=rank)] = grads[:, a * rank : (a + 1) * rank]
    inner, outer, weights = basis_in[...], basis_out[...], eigen[...]
    inner_t = inner.T
    right = fine_dot(stacked[...], outer, nn)
    parts = [right[q * rank : (q + 1) * rank] for q in range(queries)]
    scaled = [fine_dot(inner_t, part, nn) / weights for part in parts]
    back = fine_dot(jnp.concatenate(scaled, axis=0), outer, NT)
    for q in range(queries):
        turned[pl.ds(q, rank, stride=queries)] = fine_dot(inner, back[q * rank : (q + 1) * rank], nn)
    out[...] = turned[...].astype(jnp.bfloat16)


def precondition(query_grads, basis_in, basis_out, eigen):
    rank = basis_in.shape[0]
    rows = query_grads.shape[0] * rank
    return pl.pallas_call(
        precondition_kernel,
        out_shape=jax.ShapeDtypeStruct((rows, rank), jnp.bfloat16),
        in_specs=[VMEM] * 4,
        out_specs=VMEM,
        scratch_shapes=[pltpu.VMEM((rows, rank), jnp.float32)] * 2,
        cost_estimate=pl.CostEstimate(
            flops=10**10, bytes_accessed=4 * rows * rank, transcendentals=0
        ),
        compiler_params=pltpu.CompilerParams(vmem_limit_bytes=8 * MIB),
        name="precondition",
    )(query_grads, basis_in, basis_out, eigen)


def score_kernel(offsets, final, has_part, query, *refs):
    count = len(offsets)
    blocks = refs[:count]
    out, stacked, member = refs[-3:]
    rank = query.shape[1]
    queries = query.shape[0] // rank
    tokens = blocks[0].shape[1]
    me = lax.axis_index("shard")
    examples = out.shape[1]
    group = stacked.shape[1] // tokens
    lane = lax.broadcasted_iota(jnp.int32, (examples, tokens), 0)
    total = refs[count][...] if has_part else 0.0
    for first in range(0, count, group):
        for k in range(group):
            block = blocks[first + k]
            turned = jnp.dot(query[...], block[rank : 2 * rank], preferred_element_type=jnp.float32)
            inputs = block[:rank].astype(jnp.float32)
            each = jnp.sum(turned.reshape(rank, queries, tokens) * inputs[:, None, :], axis=0)
            ids = block[2 * rank :].astype(jnp.float32)[:1].astype(jnp.int32)
            owner = ids + (me ^ offsets[first + k]) * EX_DEV
            cols = pl.ds(k * tokens, tokens)
            member[:, cols] = jnp.where(lane == owner, 1.0, 0.0).astype(jnp.bfloat16)
            high = each.astype(jnp.bfloat16).astype(jnp.float32)
            mid = (each - high).astype(jnp.bfloat16).astype(jnp.float32)
            stacked[0:queries, cols] = high
            stacked[queries : 2 * queries, cols] = mid
            stacked[2 * queries :, cols] = each - high - mid
        sums = lax.dot_general(
            stacked[...].astype(jnp.bfloat16), member[...], NT, preferred_element_type=jnp.float32
        )
        total = total + (sums[:queries] + (sums[queries : 2 * queries] + sums[2 * queries :]))
    out[...] = total * SCALE if final else total


def score(query, blocks, offsets, examples, part, final):
    rank2, tokens = blocks[0].shape
    queries = query.shape[0] // query.shape[1]
    group = math.gcd(4, len(offsets))
    parts = () if part is None else (part,)
    return pl.pallas_call(
        functools.partial(score_kernel, tuple(offsets), final, bool(parts)),
        out_shape=jax.ShapeDtypeStruct((queries, examples), jnp.float32),
        in_specs=[VMEM] * (1 + len(blocks) + len(parts)),
        out_specs=VMEM,
        scratch_shapes=[
            pltpu.VMEM((3 * queries, group * tokens), jnp.float32),
            pltpu.VMEM((examples, group * tokens), jnp.bfloat16),
        ],
        cost_estimate=pl.CostEstimate(
            flops=2 * query.size * tokens * len(blocks),
            bytes_accessed=2 * rank2 * tokens * len(blocks),
            transcendentals=0,
        ),
        compiler_params=pltpu.CompilerParams(vmem_limit_bytes=4 * MIB),
    )(query, *blocks, *parts)


def on_device(
    n,
    doms,
    activations,
    out_grads,
    example_ids,
    in_factor,
    out_factor,
    query_grads,
    basis_in,
    basis_out,
    eigen,
):
    far, near, cores = grid_of(n)
    fars = [k * near * cores for k in range(1, far)]
    nears = [k * cores for k in range(1, near)]
    aligned = doms == 2 and far % 2 == 0 and in_factor.shape[1] % 128 == 0 and out_factor.shape[1] % 128 == 0
    project_all = project_paired if aligned else project_plain
    mine = project_all(n, activations, out_grads, example_ids, in_factor, out_factor)
    query = precondition(query_grads, basis_in, basis_out, eigen)
    row = {0: mine}
    for i, f in sorted(enumerate(fars), key=lambda item: (item[0] == far // 2 - 1, -item[0])):
        row[f] = moved(mine, n, f)
    rest = {o ^ m: moved(block, n, m) for m in nears for o, block in row.items()}
    steps = [row, {o ^ 1: moved(block, n, 1) for o, block in row.items()}]
    cores = {}
    for o, block in rest.items():
        cores[o ^ 1] = moved(block, n, 1)
    steps += [rest, cores]
    total = None
    for i, step in enumerate(steps):
        total = score(query, list(step.values()), list(step), EX_DEV * n, total, i == len(steps) - 1)
    return total.T


def solution(mesh):
    placed = (
        P(("dom", "shard"), None),
        P(("dom", "shard"), None),
        P(("dom", "shard"), None),
        P(None, "shard"),
        P(None, "shard"),
        P("shard", None),
        P(),
        P(),
        P(),
    )
    return jax.shard_map(
        functools.partial(on_device, mesh.shape["shard"], mesh.shape["dom"]),
        mesh=mesh,
        in_specs=placed,
        out_specs=P("dom", "shard"),
        check_vma=False,
    )
```

```python
import functools
import math

import jax
import jax.numpy as jnp
from jax import lax
from jax.experimental import pallas as pl
from jax.experimental.pallas import tpu as pltpu
from jax.sharding import PartitionSpec as P


EX_DEV = 8
SCALE = 0.00390625


def grid_of(n):
    chips = n // 2
    far = 1 << -(-int(math.log2(chips)) // 2)
    return far, chips // far, 2


def moved(value, n, offset):
    return lax.ppermute(value, "shard", [(i, i ^ offset) for i in range(n)])


NT = (((1,), (1,)), ((), ()))
VMEM = pl.BlockSpec(memory_space=pltpu.VMEM)
MIB = 1 << 20


def numbers_kernel(ids, out):
    out[...] = jnp.broadcast_to(ids[...].astype(jnp.float32), out.shape).astype(jnp.bfloat16)


def numbers_of(ids):
    return pl.pallas_call(
        numbers_kernel,
        out_shape=jax.ShapeDtypeStruct((8, ids.shape[1]), jnp.bfloat16),
        in_specs=[VMEM],
        out_specs=VMEM,
        cost_estimate=pl.CostEstimate(flops=2 * 10**10, bytes_accessed=0, transcendentals=0),
        compiler_params=pltpu.CompilerParams(vmem_limit_bytes=2 * MIB),
        name="numbers",
    )(ids)


INNER, OUTER = 0, 1


def project_kernel(keys, has_part, final, act, grad, *refs):
    count = len(keys)
    pieces = refs[:count]
    out = refs[-1]
    rank = pieces[0].shape[0]
    me = lax.axis_index("shard")
    even = lax.axis_index("dom") % 2 == 0
    part = refs[count][...] if has_part else None
    sums = [part[:, :rank], part[:, rank:]] if has_part else [0.0, 0.0]
    for piece, (first, second, kind) in zip(pieces, keys):
        src = me ^ (first if first == second else jnp.where(even, first, second))
        width = piece.shape[1]
        rows = (act, grad)[kind][:, pl.ds(pl.multiple_of(src * width, 128), width)]
        sums[kind] = sums[kind] + lax.dot_general(
            rows, piece[...], NT, preferred_element_type=jnp.float32
        )
    total = jnp.concatenate(sums, axis=1)
    if final:
        out[: 2 * rank] = total.T.astype(jnp.bfloat16)
        out[2 * rank :] = refs[count + 1][...]
    else:
        out[...] = total


def project(act, grad, pieces, keys, part, numbers):
    tokens = act.shape[0]
    rank = pieces[0].shape[0]
    extra = (() if part is None else (part,)) + (() if numbers is None else (numbers,))
    if numbers is None:
        shape = jax.ShapeDtypeStruct((tokens, 2 * rank), jnp.float32)
    else:
        shape = jax.ShapeDtypeStruct((2 * rank + 8, tokens), jnp.bfloat16)
    size = sum(piece.size for piece in pieces)
    return pl.pallas_call(
        functools.partial(project_kernel, tuple(keys), part is not None, numbers is not None),
        out_shape=shape,
        in_specs=[VMEM] * (2 + len(pieces) + len(extra)),
        out_specs=VMEM,
        cost_estimate=pl.CostEstimate(
            flops=2 * tokens * size, bytes_accessed=2 * tokens * size // rank, transcendentals=0
        ),
        compiler_params=pltpu.CompilerParams(vmem_limit_bytes=3 * MIB),
    )(act, grad, *pieces, *extra)


def project_paired(n, act, grad, ids, in_factor, out_factor):
    far, near, cores = grid_of(n)
    fars = [k * near * cores for k in range(1, far)]
    nears = [k * cores for k in range(1, near)]
    kinds = (OUTER, INNER)
    held = {(0, 0, INNER): in_factor, (0, 0, OUTER): out_factor}

    def bring(source, even, odd):
        to = (source[0] ^ even, source[1] ^ odd)
        pairs = [(i, i ^ even) for i in range(n)] + [(n + i, n + (i ^ odd)) for i in range(n)]
        for kind in kinds:
            held[(*to, kind)] = lax.ppermute(held[(*source, kind)], ("dom", "shard"), pairs)
        return to

    def cross(source):
        to = source[::-1]
        for kind in kinds:
            held[(*to, kind)] = lax.ppermute(held[(*source, kind)], "dom", [(0, 1), (1, 0)])
        return to

    own = (0, 0)
    first = [bring(own, m, m) for m in nears]
    nearest = bring(own, fars[0], fars[0])
    first.append(nearest)
    turned = [bring(nearest, m, m) for m in nears]
    middle, last = [], []
    for i in range(1, far - 1, 2):
        there = bring(own, fars[i], fars[i + 1])
        beside = [bring(there, m, m) for m in nears]
        middle += [there, *beside, cross(there)]
        last += [cross(to) for to in beside]
    for key in list(held):
        held[key[0] ^ 1, key[1] ^ 1, key[2]] = lax.ppermute(
            held[key], "shard", [(i, i ^ 1) for i in range(n)]
        )
    numbers = numbers_of(ids)
    part = None
    groups = ([own], first, middle, turned, last)
    for i, group in enumerate(groups):
        keys = [(a ^ c, b ^ c, kind) for a, b in group for c in (0, 1) for kind in kinds]
        rows = numbers if i == len(groups) - 1 else None
        part = project(act, grad, [held[key] for key in keys], keys, part, rows)
    return part


def project_plain(n, act, grad, ids, in_factor, out_factor):
    w_in, w_out = in_factor.shape[1], out_factor.shape[1]
    pieces = [jnp.concatenate([in_factor, out_factor], axis=1)]
    offsets = [0]
    step = n // 2
    while step:
        pieces += [moved(piece, n, step) for piece in pieces]
        offsets += [offset ^ step for offset in offsets]
        step //= 2
    me = lax.axis_index("shard")
    sums = [0.0, 0.0]
    for piece, offset in zip(pieces, offsets):
        src = me ^ offset
        for i, (rows, part, width) in enumerate(((act, piece[:, :w_in], w_in), (grad, piece[:, w_in:], w_out))):
            cols = lax.dynamic_slice_in_dim(rows, src * width, width, axis=1)
            sums[i] = sums[i] + lax.dot_general(part, cols, NT, preferred_element_type=jnp.float32)
    numbers = jnp.broadcast_to(ids, (8, ids.shape[1]))
    return jnp.concatenate([s.astype(jnp.bfloat16) for s in (*sums, numbers)], axis=0)


def halves_of(value):
    high = value.astype(jnp.bfloat16)
    return high, (value - high.astype(jnp.float32)).astype(jnp.bfloat16)


def fine_dot(left, right, dims):
    dot = functools.partial(lax.dot_general, dimension_numbers=dims, preferred_element_type=jnp.float32)
    (a, a_rest), (b, b_rest) = halves_of(left), halves_of(right)
    return dot(a, b) + (dot(a, b_rest) + dot(a_rest, b))


def precondition_kernel(grads, basis_in, basis_out, eigen, out, stacked, turned):
    rank = basis_in.shape[0]
    queries = grads.shape[0]
    nn = (((1,), (0,)), ((), ()))
    for a in range(rank):
        stacked[pl.ds(a, queries, stride=rank)] = grads[:, a * rank : (a + 1) * rank]
    inner, outer, weights = basis_in[...], basis_out[...], eigen[...]
    inner_t = inner.T
    right = fine_dot(stacked[...], outer, nn)
    parts = [right[q * rank : (q + 1) * rank] for q in range(queries)]
    scaled = [fine_dot(inner_t, part, nn) / weights for part in parts]
    back = fine_dot(jnp.concatenate(scaled, axis=0), outer, NT)
    for q in range(queries):
        turned[pl.ds(q, rank, stride=queries)] = fine_dot(inner, back[q * rank : (q + 1) * rank], nn)
    out[...] = turned[...].astype(jnp.bfloat16)


def precondition(query_grads, basis_in, basis_out, eigen):
    rank = basis_in.shape[0]
    rows = query_grads.shape[0] * rank
    return pl.pallas_call(
        precondition_kernel,
        out_shape=jax.ShapeDtypeStruct((rows, rank), jnp.bfloat16),
        in_specs=[VMEM] * 4,
        out_specs=VMEM,
        scratch_shapes=[pltpu.VMEM((rows, rank), jnp.float32)] * 2,
        cost_estimate=pl.CostEstimate(
            flops=10**10, bytes_accessed=4 * rows * rank, transcendentals=0
        ),
        compiler_params=pltpu.CompilerParams(vmem_limit_bytes=8 * MIB),
        name="precondition",
    )(query_grads, basis_in, basis_out, eigen)


def score_kernel(offsets, final, has_part, query, *refs):
    count = len(offsets)
    blocks = refs[:count]
    out, stacked, member = refs[-3:]
    rank = query.shape[1]
    queries = query.shape[0] // rank
    tokens = blocks[0].shape[1]
    me = lax.axis_index("shard")
    examples = out.shape[1]
    group = stacked.shape[1] // tokens
    lane = lax.broadcasted_iota(jnp.int32, (examples, tokens), 0)
    total = refs[count][...] if has_part else 0.0
    for first in range(0, count, group):
        for k in range(group):
            block = blocks[first + k]
            turned = jnp.dot(query[...], block[rank : 2 * rank], preferred_element_type=jnp.float32)
            inputs = block[:rank].astype(jnp.float32)
            each = jnp.sum(turned.reshape(rank, queries, tokens) * inputs[:, None, :], axis=0)
            ids = block[2 * rank :].astype(jnp.float32)[:1].astype(jnp.int32)
            owner = ids + (me ^ offsets[first + k]) * EX_DEV
            cols = pl.ds(k * tokens, tokens)
            member[:, cols] = jnp.where(lane == owner, 1.0, 0.0).astype(jnp.bfloat16)
            high = each.astype(jnp.bfloat16).astype(jnp.float32)
            mid = (each - high).astype(jnp.bfloat16).astype(jnp.float32)
            stacked[0:queries, cols] = high
            stacked[queries : 2 * queries, cols] = mid
            stacked[2 * queries :, cols] = each - high - mid
        sums = lax.dot_general(
            stacked[...].astype(jnp.bfloat16), member[...], NT, preferred_element_type=jnp.float32
        )
        total = total + (sums[:queries] + (sums[queries : 2 * queries] + sums[2 * queries :]))
    out[...] = total * SCALE if final else total


def score(query, blocks, offsets, examples, part, final):
    rank2, tokens = blocks[0].shape
    queries = query.shape[0] // query.shape[1]
    group = next(size for size in range(8, 0, -1) if len(offsets) % size == 0)
    parts = () if part is None else (part,)
    return pl.pallas_call(
        functools.partial(score_kernel, tuple(offsets), final, bool(parts)),
        out_shape=jax.ShapeDtypeStruct((queries, examples), jnp.float32),
        in_specs=[VMEM] * (1 + len(blocks) + len(parts)),
        out_specs=VMEM,
        scratch_shapes=[
            pltpu.VMEM((3 * queries, group * tokens), jnp.float32),
            pltpu.VMEM((examples, group * tokens), jnp.bfloat16),
        ],
        cost_estimate=pl.CostEstimate(
            flops=2 * query.size * tokens * len(blocks),
            bytes_accessed=2 * rank2 * tokens * len(blocks),
            transcendentals=0,
        ),
        compiler_params=pltpu.CompilerParams(vmem_limit_bytes=4 * MIB),
    )(query, *blocks, *parts)


def on_device(
    n,
    doms,
    activations,
    out_grads,
    example_ids,
    in_factor,
    out_factor,
    query_grads,
    basis_in,
    basis_out,
    eigen,
):
    far, near, cores = grid_of(n)
    fars = [k * near * cores for k in range(1, far)]
    nears = [k * cores for k in range(1, near)]
    aligned = doms == 2 and far % 2 == 0 and in_factor.shape[1] % 128 == 0 and out_factor.shape[1] % 128 == 0
    project_all = project_paired if aligned else project_plain
    mine = project_all(n, activations, out_grads, example_ids, in_factor, out_factor)
    query = precondition(query_grads, basis_in, basis_out, eigen)
    row = {0: mine}
    for i, f in sorted(enumerate(fars), key=lambda item: (item[0] == far // 2 - 1, -item[0])):
        row[f] = moved(mine, n, f)
    rest = {o ^ m: moved(block, n, m) for m in nears for o, block in row.items()}
    steps = [row, {o ^ 1: moved(block, n, 1) for o, block in row.items()}]
    cores = {}
    for o, block in rest.items():
        cores[o ^ 1] = moved(block, n, 1)
    *most, final = cores.items()
    steps += [{**rest, **dict(most)}, dict([final])]
    total = None
    for i, step in enumerate(steps):
        total = score(query, list(step.values()), list(step), EX_DEV * n, total, i == len(steps) - 1)
    return total.T


def solution(mesh):
    placed = (
        P(("dom", "shard"), None),
        P(("dom", "shard"), None),
        P(("dom", "shard"), None),
        P(None, "shard"),
        P(None, "shard"),
        P("shard", None),
        P(),
        P(),
        P(),
    )
    return jax.shard_map(
        functools.partial(on_device, mesh.shape["shard"], mesh.shape["dom"]),
        mesh=mesh,
        in_specs=placed,
        out_specs=P("dom", "shard"),
        check_vma=False,
    )
```
